8 devices in a mesh: dp: 1 (over z), ep: 2 (over y), sp: 4 (over x, core).
Axes of the slice: x: 2, y: 2, z: 1, core: 2. Of those that a mesh axis runs over, the one named last changes fastest.
Arguments:
- x_tokens: bfloat16 [2, 4096, 4096], P(('dp', 'ep'), 'sp')
- w_query: bfloat16 [4096, 4096], replicated
- w_key: bfloat16 [4096, 1024], replicated
- w_value: bfloat16 [4096, 1024], replicated
- w_out: bfloat16 [4096, 4096], replicated
- expert_ids: int32 [2, 4096, 2], P(('dp', 'ep'), 'sp')
- gate_probs: float32 [2, 4096, 16], P(('dp', 'ep'), 'sp')
Outputs:
- output 1: bfloat16 [2, 4096, 4096], P(('dp', 'ep'), 'sp')
- output 2: bfloat16 [4, 2, 16, 160, 4096], P(('dp', 'sp'), None, 'ep')
All inputs are finite; a program needn't handle non-finite values.
Results may differ from the reference program's by a relative error of at most 0.00895623.
Values are sent between devices in bfloat16 or wider.
A program may use at most 1 GiB of HBM per device.

```python
import math
import jax
import jax.numpy as jnp
from jax import lax

TOK_DEV = 1024
D_MODEL = 4096
N_HEADS = 32
KV_HEADS = 8
HEAD_DIM = 128
EXPERTS = 16
TOP_K = 2
EP_SIZE = 2
SP_SIZE = 4
CAPACITY = 160


def draw_expert_ids(key_ids, key_hot, key_coin, seq_len):
    hot_expert = jax.random.randint(key_hot, (EP_SIZE, 1, 1), 0, EXPERTS)
    coin_flip = jax.random.randint(key_coin, (EP_SIZE, seq_len, 1), 0, 4)
    even_pos = (jnp.arange(seq_len) % 2 == 0)[None, :, None]
    expert_axis = jnp.arange(EXPERTS)[None, None, :]
    forced = ((coin_flip > 0) | even_pos) & (expert_axis == hot_expert)
    raw_score = jax.random.randint(key_ids, (EP_SIZE, seq_len, EXPERTS), 0, 2 ** 20)
    int_score = (raw_score + jnp.where(forced, 2 ** 21, 0)) * EXPERTS + expert_axis
    top_scores, expert_ids = lax.top_k(int_score, TOP_K)
    return expert_ids.astype(jnp.int32)


def setup_inputs(seed: int = 0, part: int = 0) -> dict:
    shared_key, data_key = jax.random.split(jax.random.key(seed))
    part_key = jax.random.fold_in(data_key, part)
    key_x, key_ids, key_hot, key_coin, key_gate = jax.random.split(part_key, 5)
    key_q, key_k, key_v, key_o = jax.random.split(shared_key, 4)
    seq_len = TOK_DEV * SP_SIZE
    q_width = N_HEADS * HEAD_DIM
    kv_width = KV_HEADS * HEAD_DIM
    sharpness = math.log(seq_len / 8.0) ** 0.25
    x_tokens = jax.random.normal(key_x, (EP_SIZE, seq_len, D_MODEL), jnp.float32).astype(jnp.bfloat16)
    w_query = (jax.random.normal(key_q, (D_MODEL, q_width), jnp.float32) * (sharpness / math.sqrt(D_MODEL))).astype(jnp.bfloat16)
    w_key = (jax.random.normal(key_k, (D_MODEL, kv_width), jnp.float32) * (sharpness / math.sqrt(D_MODEL))).astype(jnp.bfloat16)
    w_value = (jax.random.normal(key_v, (D_MODEL, kv_width), jnp.float32) * (1.0 / math.sqrt(D_MODEL))).astype(jnp.bfloat16)
    w_out = (jax.random.normal(key_o, (q_width, D_MODEL), jnp.float32) * (2.0 / math.sqrt(q_width))).astype(jnp.bfloat16)
    expert_ids = draw_expert_ids(key_ids, key_hot, key_coin, seq_len)
    gate_probs = jax.random.uniform(key_gate, (EP_SIZE, seq_len, EXPERTS), jnp.float32, 0.25, 1.75)
    return {'x_tokens': x_tokens, 'w_query': w_query, 'w_key': w_key, 'w_value': w_value, 'w_out': w_out, 'expert_ids': expert_ids, 'gate_probs': gate_probs}


def attend(q_rows, k_all, v_all):
    n_query, kv_count, group_size, head_dim = q_rows.shape
    seq_len = k_all.shape[0]
    q_block = n_query
    while q_block % 2 == 0 and q_block > 8 and q_block * kv_count * group_size * seq_len > 2 ** 24:
        q_block = q_block // 2
    n_blocks = n_query // q_block
    k_wide = k_all.astype(jnp.float32)
    v_wide = v_all.astype(jnp.float32)
    key_pos = jnp.arange(seq_len)
    inv_sqrt = 1.0 / math.sqrt(head_dim)

    def one_block(block_in):
        blk_index, q_blk = block_in
        scores = jnp.einsum('qkgd,skd->kgqs', q_blk.astype(jnp.float32), k_wide) * inv_sqrt
        query_pos = blk_index * q_block + jnp.arange(q_block)
        scores = jnp.where(key_pos[None, :] <= query_pos[:, None], scores, -jnp.inf)
        prob_bf = jax.nn.softmax(scores, axis=-1).astype(jnp.bfloat16)
        block_out = jnp.einsum('kgqs,skd->qkgd', prob_bf.astype(jnp.float32), v_wide)
        return block_out.astype(jnp.bfloat16)

    block_outs = lax.map(one_block, (jnp.arange(n_blocks), q_rows.reshape(n_blocks, q_block, kv_count, group_size, head_dim)))
    return block_outs.reshape(n_query, kv_count, group_size, head_dim)


def dispatch_block(hidden, ids_rows, gate_rows):
    n_pairs = TOK_DEV * TOP_K
    gate_pick = jnp.take_along_axis(gate_rows, ids_rows, axis=1).reshape(n_pairs)
    flat_ids = ids_rows.reshape(n_pairs)
    one_hot = (flat_ids[:, None] == jnp.arange(EXPERTS)[None, :]).astype(jnp.int32)
    slot_rank = jnp.sum(jnp.cumsum(one_hot, axis=0) * one_hot, axis=1) - 1
    dest_row = jnp.where(slot_rank < CAPACITY, flat_ids * CAPACITY + slot_rank, EXPERTS * CAPACITY)
    pair_tok = jnp.arange(n_pairs, dtype=jnp.int32) // TOP_K
    slot_tok = jnp.full((EXPERTS * CAPACITY,), TOK_DEV, jnp.int32).at[dest_row].set(pair_tok, mode='drop')
    slot_gate = jnp.zeros((EXPERTS * CAPACITY,), jnp.float32).at[dest_row].set(gate_pick, mode='drop')
    padded = jnp.concatenate([hidden, jnp.zeros((1, D_MODEL), hidden.dtype)], axis=0)
    slot_rows = (jnp.take(padded, slot_tok, axis=0).astype(jnp.float32) * slot_gate[:, None]).astype(jnp.bfloat16)
    return slot_rows.reshape(EXPERTS, CAPACITY, D_MODEL)


def reference(x_tokens, w_query, w_key, w_value, w_out, expert_ids, gate_probs):
    seq_len = TOK_DEV * SP_SIZE
    group_size = N_HEADS // KV_HEADS

    def one_seq(x_seq):
        q_seq = jnp.dot(x_seq, w_query, preferred_element_type=jnp.float32).astype(jnp.bfloat16)
        k_seq = jnp.dot(x_seq, w_key, preferred_element_type=jnp.float32).astype(jnp.bfloat16)
        v_seq = jnp.dot(x_seq, w_value, preferred_element_type=jnp.float32).astype(jnp.bfloat16)
        attn_out = attend(q_seq.reshape(seq_len, KV_HEADS, group_size, HEAD_DIM), k_seq.reshape(seq_len, KV_HEADS, HEAD_DIM), v_seq.reshape(seq_len, KV_HEADS, HEAD_DIM))
        mixed = jnp.dot(attn_out.reshape(seq_len, N_HEADS * HEAD_DIM), w_out, preferred_element_type=jnp.float32)
        return (x_seq.astype(jnp.float32) + mixed).astype(jnp.bfloat16)

    hidden = lax.map(one_seq, x_tokens)
    per_source = jax.vmap(jax.vmap(dispatch_block))(hidden.reshape(EP_SIZE, SP_SIZE, TOK_DEV, D_MODEL), expert_ids.reshape(EP_SIZE, SP_SIZE, TOK_DEV, TOP_K), gate_probs.reshape(EP_SIZE, SP_SIZE, TOK_DEV, EXPERTS))
    expert_buf = jnp.transpose(per_source, (1, 0, 2, 3, 4))
    return hidden, expert_buf
```

```python
import functools
import math
import jax
import jax.numpy as jnp
from jax import lax
from jax.experimental import pallas as pl
from jax.experimental.pallas import tpu as pltpu
from jax.sharding import PartitionSpec as P

HEAD_DIM = 128
KEY_BLOCK = 512
NEG = -0.7 * 3.4028235e38
BF16 = jnp.bfloat16
F32 = jnp.float32


def capacity_of(tok_dev, top_k, experts):
    return max(8, 8 * ((5 * tok_dev * top_k + 32 * experts - 1) // (32 * experts)))


def attend_kernel(group, diag_start, counts, q_ref, kd_ref, vd_ref, ko_ref, vo_ref, ka_ref, va_ref, kb_ref, vb_ref, o_ref, acc_ref):
    rows = q_ref.shape[0]
    scale = math.log2(math.e) / math.sqrt(HEAD_DIM)
    queries = [q_ref[:, h * HEAD_DIM:(h + 1) * HEAD_DIM] for h in range(group)]
    acc_ref[...] = jnp.zeros_like(acc_ref)

    def fold(k_blk, v_blk, state, mask):
        new_state = []
        for h in range(group):
            m_old, l_old = state[2 * h], state[2 * h + 1]
            s = lax.dot_general(k_blk, queries[h], (((1,), (1,)), ((), ())), preferred_element_type=F32)
            if mask is not None:
                s = jnp.where(mask, s, NEG)
            m_new = jnp.maximum(m_old, jnp.max(s, axis=0, keepdims=True))
            p = jnp.exp2(s * scale - m_new * scale)
            alpha = jnp.exp2((m_old - m_new) * scale)
            l_new = l_old * alpha + jnp.sum(p, axis=0, keepdims=True)
            pv = lax.dot_general(v_blk, p.astype(BF16), (((0,), (0,)), ((), ())), preferred_element_type=F32)
            acc_ref[h] = acc_ref[h] * alpha + pv
            new_state += [m_new, l_new]
        return tuple(new_state)

    def full(k_ref, v_ref, n_blocks, state):
        def step(i, st):
            start = pl.multiple_of(i * KEY_BLOCK, KEY_BLOCK)
            return fold(k_ref[pl.ds(start, KEY_BLOCK), :], v_ref[pl.ds(start, KEY_BLOCK), :], st, None)
        return lax.fori_loop(0, n_blocks, step, state)

    state = tuple(jnp.full((1, rows), NEG, F32) if i % 2 == 0 else jnp.zeros((1, rows), F32) for i in range(2 * group))
    per_block = ko_ref.shape[0] // KEY_BLOCK
    key_i = lax.broadcasted_iota(jnp.int32, (rows, rows), 0)
    qry_i = lax.broadcasted_iota(jnp.int32, (rows, rows), 1)
    state = fold(kd_ref[diag_start:diag_start + rows, :], vd_ref[diag_start:diag_start + rows, :], state, key_i <= qry_i)
    if diag_start:
        state = fold(kd_ref[:diag_start, :], vd_ref[:diag_start, :], state, None)
    state = full(ko_ref, vo_ref, counts[0] * per_block, state)
    state = full(ka_ref, va_ref, counts[1] * per_block, state)
    state = full(kb_ref, vb_ref, counts[1] * per_block, state)
    for h in range(group):
        o_t = acc_ref[h] * (1.0 / state[2 * h + 1])
        o_ref[:, h * HEAD_DIM:(h + 1) * HEAD_DIM] = o_t.T.astype(BF16)


def attend(counts, q_chunk, kvs, diag_start, kv_heads):
    rows, width = q_chunk.shape
    group = width // HEAD_DIM // kv_heads
    block = kvs[0].shape[0]
    kv_spec = pl.BlockSpec((block, HEAD_DIM), lambda g, c: (0, g))
    q_spec = pl.BlockSpec((rows, group * HEAD_DIM), lambda g, c: (0, g))
    return pl.pallas_call(
        functools.partial(attend_kernel, group, diag_start),
        grid_spec=pltpu.PrefetchScalarGridSpec(
            num_scalar_prefetch=1, grid=(kv_heads,), in_specs=[q_spec] + [kv_spec] * 8, out_specs=q_spec,
            scratch_shapes=[pltpu.VMEM((group, HEAD_DIM, rows), F32)]),
        out_shape=jax.ShapeDtypeStruct((rows, width), BF16),
        cost_estimate=pl.CostEstimate(flops=4 * rows * width * 3 * block, bytes_accessed=2 * (2 * rows * width + 8 * block * kv_heads * HEAD_DIM), transcendentals=rows * width // HEAD_DIM * 3 * block),
        compiler_params=pltpu.CompilerParams(dimension_semantics=('arbitrary',)),
        name='attend',
    )(counts, q_chunk, *kvs)


def build_kernel(capacity, n_parts, aliased, where, slot_ref, gate_ref, *refs):
    parts, (o_ref, pick_ref, scale_ref) = refs[:n_parts], refs[-3:]
    experts, tokens = slot_ref.shape

    @pl.when(pl.program_id(0) == 0)
    def _():
        rank = lax.broadcasted_iota(jnp.int32, (capacity, tokens), 0)
        for e in range(experts):
            hit = slot_ref[e:e + 1, :] == rank
            pick_ref[e * capacity:(e + 1) * capacity, :] = jnp.where(hit, 1.0, 0.0).astype(BF16)
            picked = jnp.sum(jnp.where(hit, gate_ref[e:e + 1, :], 0.0), axis=1, keepdims=True)
            scale_ref[e * capacity:(e + 1) * capacity, :] = jnp.broadcast_to(picked, (capacity, HEAD_DIM))

    for e in range(experts):
        lo, hi, at = e * capacity, (e + 1) * capacity, 0
        total = None
        for part in parts:
            n = part.shape[0]
            term = jnp.dot(pick_ref[lo:hi, at:at + n], part[...], preferred_element_type=F32)
            total = term if total is None else total + term
            at += n
        o_ref[0, 0, e] = (total * scale_ref[lo:hi, 0:1]).astype(BF16)


def build(where, slots, gates, parts, capacity, prior=None, col=512):
    experts, tokens = slots.shape
    d_model = parts[0].shape[1]
    fixed = pl.BlockSpec((experts, tokens), lambda n, w: (0, 0))
    in_specs = [fixed, fixed] + [pl.BlockSpec((p.shape[0], col), lambda n, w: (0, n)) for p in parts]
    args = [slots, gates, *parts]
    aliases = {}
    if prior is not None:
        in_specs.append(pl.BlockSpec(memory_space=pl.ANY))
        args.append(prior)
        aliases = {len(args): 0}
    return pl.pallas_call(
        functools.partial(build_kernel, capacity, len(parts), prior is not None),
        grid_spec=pltpu.PrefetchScalarGridSpec(
            num_scalar_prefetch=1, grid=(d_model // col,), in_specs=in_specs,
            out_specs=pl.BlockSpec((1, 1, experts, capacity, col), lambda n, w: (0, w[0], 0, 0, n)),
            scratch_shapes=[pltpu.VMEM((experts * capacity, tokens), BF16), pltpu.VMEM((experts * capacity, HEAD_DIM), F32)]),
        out_shape=jax.ShapeDtypeStruct((1, 2, experts, capacity, d_model), BF16),
        input_output_aliases=aliases,
        cost_estimate=pl.CostEstimate(flops=2 * experts * capacity * tokens * d_model, bytes_accessed=2 * d_model * (tokens + experts * capacity), transcendentals=0),
        compiler_params=pltpu.CompilerParams(dimension_semantics=('arbitrary',)),
        name='build',
    )(where, *args)


def slots_of(ids_rows, experts):
    tok_dev = ids_rows.shape[0]
    routed = jnp.any(ids_rows[:, :, None] == jnp.arange(experts)[None, None, :], axis=1)
    earlier = jnp.arange(tok_dev)[None, :] < jnp.arange(tok_dev)[:, None]
    rank = jnp.dot(earlier.astype(BF16), routed.astype(BF16), preferred_element_type=F32)
    return jnp.where(routed, rank, -1.0).astype(jnp.int32).T


def solution(mesh):
    sp_size = mesh.shape['sp']
    ep_size = mesh.shape['ep']
    pairs = [(i, i ^ 1) for i in range(sp_size)]
    across = [(0, 2), (1, 3)]
    ep_same = [(e * sp_size + s, (1 - e) * sp_size + s) for e in range(ep_size) for s in range(sp_size)]
    ep_cross = [(e * sp_size + s, (1 - e) * sp_size + (s ^ 1)) for e in range(ep_size) for s in range(sp_size)]

    def swap(a):
        return lax.ppermute(a, 'sp', pairs)

    def per_device(x_blk, w_query, w_key, w_value, w_out, ids_blk, gate_blk):
        x_own = x_blk[0]
        tok_dev, d_model = x_own.shape
        half = tok_dev // 2
        chunk = half // 2
        kv_heads = w_key.shape[1] // HEAD_DIM
        experts = gate_blk.shape[2]
        capacity = capacity_of(tok_dev, ids_blk.shape[2], experts)
        ep = lax.axis_index('ep')
        sp = lax.axis_index('sp')

        x_upper = swap(x_own[half:])
        k_own = jnp.dot(x_own, w_key, preferred_element_type=F32).astype(BF16)
        v_own = jnp.dot(x_own, w_value, preferred_element_type=F32).astype(BF16)
        k_a, v_a = lax.ppermute(k_own, 'sp', across), lax.ppermute(v_own, 'sp', across)
        k_mate, v_mate = swap(k_own), swap(v_own)
        k_b, v_b = swap(k_a), swap(v_a)
        q_low = jnp.dot(x_own[:half], w_query, preferred_element_type=F32).astype(BF16)
        q_upp = jnp.dot(x_upper, w_query, preferred_element_type=F32).astype(BF16)

        far = (sp >= 2).astype(jnp.int32)
        odd = (sp % 2).astype(jnp.int32)
        counts_low = jnp.stack([odd, far])
        counts_upp = jnp.stack([1 - odd, far])

        ids_other = lax.ppermute(ids_blk[0], ('ep', 'sp'), ep_same)
        gates_other = lax.ppermute(gate_blk[0], ('ep', 'sp'), ep_same)
        local = experts // ep_size

        def mine(a):
            return lax.dynamic_slice_in_dim(a, ep * local, local, 0)

        slots_own, gates_own = mine(slots_of(ids_blk[0], experts)), mine(gate_blk[0].T)
        slots_oth, gates_oth = mine(slots_of(ids_other, experts)), mine(gates_other.T)

        own_rows, other_rows = [], []
        for c in range(4):
            lower = c < 2
            at = (c % 2) * chunk
            q_c = lax.slice_in_dim(q_low if lower else q_upp, at, at + chunk, axis=0)
            x_c = lax.slice_in_dim(x_own if lower else x_upper, at, at + chunk, axis=0)
            diag = (k_own, v_own) if lower else (k_mate, v_mate)
            other = (k_mate, v_mate) if lower else (k_own, v_own)
            o_c = attend(counts_low if lower else counts_upp, q_c, (*diag, *other, k_a, v_a, k_b, v_b), c * chunk, kv_heads)
            mixed = jnp.dot(o_c, w_out, preferred_element_type=F32)
            h_c = (x_c.astype(F32) + mixed).astype(BF16)
            own_rows.append(h_c if lower else swap(h_c))
            other_rows.append(lax.ppermute(h_c, ('ep', 'sp'), ep_same if lower else ep_cross))
        hidden = jnp.concatenate(own_rows, axis=0)
        buf = build(ep[None].astype(jnp.int32), slots_own, gates_own, [hidden], capacity)
        buf = build((1 - ep)[None].astype(jnp.int32), slots_oth, gates_oth, other_rows, capacity, prior=buf)
        return hidden[None], buf

    seq_spec = P(('dp', 'ep'), 'sp', None)
    buf_spec = P(('dp', 'sp'), None, 'ep', None, None)
    return jax.shard_map(per_device, mesh=mesh, in_specs=(seq_spec, P(), P(), P(), P(), seq_spec, seq_spec), out_specs=(seq_spec, buf_spec), check_vma=False)
```

```python
import functools
import math
import jax
import jax.numpy as jnp
from jax import lax
from jax.experimental import pallas as pl
from jax.experimental.pallas import tpu as pltpu
from jax.sharding import PartitionSpec as P

HEAD_DIM = 128
KEY_BLOCK = 512
NEG = -0.7 * 3.4028235e38
BF16 = jnp.bfloat16
F32 = jnp.float32


def capacity_of(tok_dev, top_k, experts):
    return max(8, 8 * ((5 * tok_dev * top_k + 32 * experts - 1) // (32 * experts)))


def attend_kernel(group, diag_start, counts, q_ref, *refs):
    (k_far0, v_far0, k_far1, v_far1, k_oth, v_oth, k_own, v_own, o_ref, k_buf, v_buf, s_ref, acc_ref, sems) = refs
    g, n_g = pl.program_id(0), pl.num_programs(0)
    rows = q_ref.shape[0]
    block = k_own.shape[0]
    oth, far = counts[0], counts[1]
    scale = math.log2(math.e) / math.sqrt(HEAD_DIM)
    own_at = far * (2 * block) + oth * block
    own_len = diag_start + rows
    rest = own_len % KEY_BLOCK
    last_len = rest if rest else KEY_BLOCK
    n_full = (own_at + own_len - last_len) // KEY_BLOCK

    def copies(head, slot):
        def pair(k_src, v_src, at, n):
            cols = pl.ds(head * HEAD_DIM, HEAD_DIM)
            at = pl.multiple_of(at, 256)
            return [pltpu.make_async_copy(k_src.at[pl.ds(0, n), cols], k_buf.at[slot, pl.ds(at, n), :], sems.at[slot, 0]),
                    pltpu.make_async_copy(v_src.at[pl.ds(0, n), cols], v_buf.at[slot, pl.ds(at, n), :], sems.at[slot, 1])]
        return (pair(k_far0, v_far0, 0, block) + pair(k_far1, v_far1, block, block),
                pair(k_oth, v_oth, far * (2 * block), block), pair(k_own, v_own, own_at, own_len))

    def each(head, slot, act):
        far_c, oth_c, own_c = copies(head, slot)

        @pl.when(far > 0)
        def _():
            for c in far_c:
                act(c)

        @pl.when(oth > 0)
        def _():
            for c in oth_c:
                act(c)

        for c in own_c:
            act(c)

    slot = lax.rem(g, 2)

    @pl.when(g == 0)
    def _():
        each(0, 0, lambda c: c.start())

    @pl.when(g + 1 < n_g)
    def _():
        each(g + 1, 1 - slot, lambda c: c.start())

    each(g, slot, lambda c: c.wait())
    acc_ref[...] = jnp.zeros_like(acc_ref)

    def score(i, h, n, masked):
        k_blk = k_buf[slot, pl.ds(pl.multiple_of(i * KEY_BLOCK, KEY_BLOCK), n), :]
        s = lax.dot_general(k_blk, q_ref[:, h * HEAD_DIM:(h + 1) * HEAD_DIM], (((1,), (1,)), ((), ())), preferred_element_type=F32)
        if masked:
            key_i = lax.broadcasted_iota(jnp.int32, (n, rows), 0)
            qry_i = lax.broadcasted_iota(jnp.int32, (n, rows), 1) + (last_len - rows)
            s = jnp.where(key_i <= qry_i, s, NEG)
        s_ref[h % 2, :n, :] = s
        return jnp.max(s, axis=0, keepdims=True)

    def value(i, h, n, top, m_old, l_old):
        m_new = jnp.maximum(m_old, top)
        v_blk = v_buf[slot, pl.ds(pl.multiple_of(i * KEY_BLOCK, KEY_BLOCK), n), :]
        p = jnp.exp2(s_ref[h % 2, :n, :] * scale - m_new * scale)
        alpha = jnp.exp2((m_old - m_new) * scale)
        l_new = l_old * alpha + jnp.sum(p, axis=0, keepdims=True)
        pv = lax.dot_general(v_blk, p.astype(BF16), (((0,), (0,)), ((), ())), preferred_element_type=F32)
        acc_ref[h] = acc_ref[h] * alpha + pv
        return m_new, l_new

    def step(i, carry):
        top, ms, ls = carry
        ms, ls = list(ms), list(ls)
        for h in range(group):
            if h + 1 < group:
                top_next = score(i, h + 1, KEY_BLOCK, False)
            else:
                top_next = score(i + 1, 0, KEY_BLOCK, False)
            ms[h], ls[h] = value(i, h, KEY_BLOCK, top, ms[h], ls[h])
            top = top_next
        return top, tuple(ms), tuple(ls)

    m0 = tuple(jnp.full((1, rows), NEG, F32) for _ in range(group))
    l0 = tuple(jnp.zeros((1, rows), F32) for _ in range(group))
    top = lax.cond(n_full > 0, lambda: score(0, 0, KEY_BLOCK, False), lambda: jnp.zeros((1, rows), F32))
    _, ms, ls = lax.fori_loop(0, n_full, step, (top, m0, l0))
    top = score(n_full, 0, last_len, True)
    for h in range(group):
        if h + 1 < group:
            top_next = score(n_full, h + 1, last_len, True)
        _, l_end = value(n_full, h, last_len, top, ms[h], ls[h])
        top = top_next
        o_t = acc_ref[h] * (1.0 / l_end)
        o_ref[:, h * HEAD_DIM:(h + 1) * HEAD_DIM] = o_t.T.astype(BF16)


def attend(counts, q_chunk, own, other, far0, far1, diag_start, kv_heads):
    rows, width = q_chunk.shape
    group = width // HEAD_DIM // kv_heads
    block = own[0].shape[0]
    q_spec = pl.BlockSpec((rows, group * HEAD_DIM), lambda g, c: (0, g))
    return pl.pallas_call(
        functools.partial(attend_kernel, group, diag_start),
        grid_spec=pltpu.PrefetchScalarGridSpec(
            num_scalar_prefetch=1, grid=(kv_heads,), in_specs=[q_spec] + [pl.BlockSpec(memory_space=pltpu.HBM)] * 8, out_specs=q_spec,
            scratch_shapes=[pltpu.VMEM((2, 4 * block, HEAD_DIM), BF16), pltpu.VMEM((2, 4 * block, HEAD_DIM), BF16),
                            pltpu.VMEM((2, KEY_BLOCK, rows), F32), pltpu.VMEM((group, HEAD_DIM, rows), F32),
                            pltpu.SemaphoreType.DMA((2, 2))]),
        out_shape=jax.ShapeDtypeStruct((rows, width), BF16),
        cost_estimate=pl.CostEstimate(flops=4 * rows * width * 3 * block, bytes_accessed=2 * (2 * rows * width + 8 * block * kv_heads * HEAD_DIM), transcendentals=rows * width // HEAD_DIM * 3 * block),
        compiler_params=pltpu.CompilerParams(dimension_semantics=('arbitrary',)),
        name='attend',
    )(counts, q_chunk, *far0, *far1, *other, *own)


def build_kernel(capacity, n_parts, aliased, where, slot_ref, gate_ref, *refs):
    parts, (o_ref, pick_ref, scale_ref) = refs[:n_parts], refs[-3:]
    experts, tokens = slot_ref.shape

    @pl.when(pl.program_id(0) == 0)
    def _():
        rank = lax.broadcasted_iota(jnp.int32, (capacity, tokens), 0)
        for e in range(experts):
            hit = slot_ref[e:e + 1, :] == rank
            pick_ref[e * capacity:(e + 1) * capacity, :] = jnp.where(hit, 1.0, 0.0).astype(BF16)
            picked = jnp.sum(jnp.where(hit, gate_ref[e:e + 1, :], 0.0), axis=1, keepdims=True)
            scale_ref[e * capacity:(e + 1) * capacity, :] = jnp.broadcast_to(picked, (capacity, HEAD_DIM))

    for e in range(experts):
        lo, hi, at = e * capacity, (e + 1) * capacity, 0
        total = None
        for part in parts:
            n = part.shape[0]
            term = jnp.dot(pick_ref[lo:hi, at:at + n], part[...], preferred_element_type=F32)
            total = term if total is None else total + term
            at += n
        o_ref[0, 0, e] = (total * scale_ref[lo:hi, 0:1]).astype(BF16)


def build(where, slots, gates, parts, capacity, prior=None, col=512):
    experts, tokens = slots.shape
    d_model = parts[0].shape[1]
    fixed = pl.BlockSpec((experts, tokens), lambda n, w: (0, 0))
    in_specs = [fixed, fixed] + [pl.BlockSpec((p.shape[0], col), lambda n, w: (0, n)) for p in parts]
    args = [slots, gates, *parts]
    aliases = {}
    if prior is not None:
        in_specs.append(pl.BlockSpec(memory_space=pl.ANY))
        args.append(prior)
        aliases = {len(args): 0}
    return pl.pallas_call(
        functools.partial(build_kernel, capacity, len(parts), prior is not None),
        grid_spec=pltpu.PrefetchScalarGridSpec(
            num_scalar_prefetch=1, grid=(d_model // col,), in_specs=in_specs,
            out_specs=pl.BlockSpec((1, 1, experts, capacity, col), lambda n, w: (0, w[0], 0, 0, n)),
            scratch_shapes=[pltpu.VMEM((experts * capacity, tokens), BF16), pltpu.VMEM((experts * capacity, HEAD_DIM), F32)]),
        out_shape=jax.ShapeDtypeStruct((1, 2, experts, capacity, d_model), BF16),
        input_output_aliases=aliases,
        cost_estimate=pl.CostEstimate(flops=2 * experts * capacity * tokens * d_model, bytes_accessed=2 * d_model * (tokens + experts * capacity), transcendentals=0),
        compiler_params=pltpu.CompilerParams(dimension_semantics=('arbitrary',)),
        name='build',
    )(where, *args)


def slots_of(ids_rows, experts):
    tok_dev = ids_rows.shape[0]
    routed = jnp.any(ids_rows[:, :, None] == jnp.arange(experts)[None, None, :], axis=1)
    earlier = jnp.arange(tok_dev)[None, :] < jnp.arange(tok_dev)[:, None]
    rank = jnp.dot(earlier.astype(BF16), routed.astype(BF16), preferred_element_type=F32)
    return jnp.where(routed, rank, -1.0).astype(jnp.int32).T


def solution(mesh):
    sp_size = mesh.shape['sp']
    ep_size = mesh.shape['ep']
    pairs = [(i, i ^ 1) for i in range(sp_size)]
    across = [(0, 2), (1, 3)]
    ep_same = [(e * sp_size + s, (1 - e) * sp_size + s) for e in range(ep_size) for s in range(sp_size)]
    ep_cross = [(e * sp_size + s, (1 - e) * sp_size + (s ^ 1)) for e in range(ep_size) for s in range(sp_size)]

    def swap(a):
        return lax.ppermute(a, 'sp', pairs)

    def per_device(x_blk, w_query, w_key, w_value, w_out, ids_blk, gate_blk):
        x_own = x_blk[0]
        tok_dev, d_model = x_own.shape
        half = tok_dev // 2
        chunk = half // 2
        kv_heads = w_key.shape[1] // HEAD_DIM
        experts = gate_blk.shape[2]
        capacity = capacity_of(tok_dev, ids_blk.shape[2], experts)
        ep = lax.axis_index('ep')
        sp = lax.axis_index('sp')

        x_upper = swap(x_own[half:])
        k_own = jnp.dot(x_own, w_key, preferred_element_type=F32).astype(BF16)
        v_own = jnp.dot(x_own, w_value, preferred_element_type=F32).astype(BF16)
        k_a, v_a = lax.ppermute(k_own, 'sp', across), lax.ppermute(v_own, 'sp', across)
        k_mate, v_mate = swap(k_own), swap(v_own)
        k_b, v_b = swap(k_a), swap(v_a)
        q_low = jnp.dot(x_own[:half], w_query, preferred_element_type=F32).astype(BF16)
        q_upp = jnp.dot(x_upper, w_query, preferred_element_type=F32).astype(BF16)

        far = (sp >= 2).astype(jnp.int32)
        odd = (sp % 2).astype(jnp.int32)
        counts_low = jnp.stack([odd, far])
        counts_upp = jnp.stack([1 - odd, far])

        ids_other = lax.ppermute(ids_blk[0], ('ep', 'sp'), ep_same)
        gates_other = lax.ppermute(gate_blk[0], ('ep', 'sp'), ep_same)
        local = experts // ep_size

        def mine(a):
            return lax.dynamic_slice_in_dim(a, ep * local, local, 0)

        slots_own, gates_own = mine(slots_of(ids_blk[0], experts)), mine(gate_blk[0].T)
        slots_oth, gates_oth = mine(slots_of(ids_other, experts)), mine(gates_other.T)

        own_rows, other_rows = [], []
        for c in range(4):
            lower = c < 2
            at = (c % 2) * chunk
            q_c = lax.slice_in_dim(q_low if lower else q_upp, at, at + chunk, axis=0)
            x_c = lax.slice_in_dim(x_own if lower else x_upper, at, at + chunk, axis=0)
            diag = (k_own, v_own) if lower else (k_mate, v_mate)
            other = (k_mate, v_mate) if lower else (k_own, v_own)
            o_c = attend(counts_low if lower else counts_upp, q_c, diag, other, (k_a, v_a), (k_b, v_b), c * chunk, kv_heads)
            mixed = jnp.dot(o_c, w_out, preferred_element_type=F32)
            h_c = (x_c.astype(F32) + mixed).astype(BF16)
            own_rows.append(h_c if lower else swap(h_c))
            other_rows.append(lax.ppermute(h_c, ('ep', 'sp'), ep_same if lower else ep_cross))
        hidden = jnp.concatenate(own_rows, axis=0)
        buf = build(ep[None].astype(jnp.int32), slots_own, gates_own, [hidden], capacity)
        buf = build((1 - ep)[None].astype(jnp.int32), slots_oth, gates_oth, other_rows, capacity, prior=buf)
        return hidden[None], buf

    seq_spec = P(('dp', 'ep'), 'sp', None)
    buf_spec = P(('dp', 'sp'), None, 'ep', None, None)
    return jax.shard_map(per_device, mesh=mesh, in_specs=(seq_spec, P(), P(), P(), P(), seq_spec, seq_spec), out_specs=(seq_spec, buf_spec), check_vma=False)
```

```python
import functools
import math
import jax
import jax.numpy as jnp
from jax import lax
from jax.experimental import pallas as pl
from jax.experimental.pallas import tpu as pltpu
from jax.sharding import PartitionSpec as P

HEAD_DIM = 128
TILE = 256
NEG = -0.7 * 3.4028235e38
BF16 = jnp.bfloat16
F32 = jnp.float32


def capacity_of(tok_dev, top_k, experts):
    return max(8, 8 * ((5 * tok_dev * top_k + 32 * experts - 1) // (32 * experts)))


def fold_blocks(items, q_ref, s_ref, acc_ref, m_l):
    rows = q_ref.shape[0]
    scale = math.log2(math.e) / math.sqrt(HEAD_DIM)

    def score(idx, at):
        h, k_ref, _, start, _, masked = items[idx]
        s = lax.dot_general(k_ref[start + at:start + at + TILE, :], q_ref[:, h * HEAD_DIM:(h + 1) * HEAD_DIM], (((1,), (1,)), ((), ())), preferred_element_type=F32)
        if masked is not None and at + TILE > masked:
            key_i = lax.broadcasted_iota(jnp.int32, (TILE, rows), 0) + (at - masked)
            qry_i = lax.broadcasted_iota(jnp.int32, (TILE, rows), 1)
            s = jnp.where(key_i <= qry_i, s, NEG)
        s_ref[idx % 2, at:at + TILE, :] = s
        return jnp.max(s, axis=0, keepdims=True)

    def join(top, t):
        return t if top is None else jnp.maximum(top, t)

    top = None
    for at in range(0, items[0][4], TILE):
        top = join(top, score(0, at))
    for idx, (h, _, v_ref, start, n, _) in enumerate(items):
        n_next = items[idx + 1][4] if idx + 1 < len(items) else 0
        m_old, l_old = m_l[h]
        m_new = jnp.maximum(m_old, top)
        shift = m_new * scale
        alpha = jnp.exp2((m_old - m_new) * scale)
        l_new = l_old * alpha
        top, pv = None, None
        for at in range(0, max(n, n_next), TILE):
            if at < n_next:
                top = join(top, score(idx + 1, at))
            if at < n:
                p = jnp.exp2(s_ref[idx % 2, at:at + TILE, :] * scale - shift)
                l_new = l_new + jnp.sum(p, axis=0, keepdims=True)
                term = lax.dot_general(v_ref[start + at:start + at + TILE, :], p.astype(BF16), (((0,), (0,)), ((), ())), preferred_element_type=F32)
                pv = term if pv is None else pv + term
        acc_ref[h] = acc_ref[h] * alpha + pv
        m_l[h] = (m_new, l_new)
    return m_l


def near_kernel(group, diag_start, counts, q_ref, k_oth, v_oth, k_own, v_own, acc_ref, ml_ref, s_ref):
    rows = q_ref.shape[0]
    acc = acc_ref.at[0]
    acc[...] = jnp.zeros_like(acc)
    ml_ref[0, :group] = jnp.full((group, rows), NEG, F32)
    ml_ref[0, group:] = jnp.zeros((group, rows), F32)

    def run(items):
        m_l = [(ml_ref[0, h:h + 1], ml_ref[0, group + h:group + h + 1]) for h in range(group)]
        for h, (m, l) in enumerate(fold_blocks(items, q_ref, s_ref, acc, m_l)):
            ml_ref[0, h:h + 1] = m
            ml_ref[0, group + h:group + h + 1] = l

    @pl.when(counts[0] > 0)
    def _():
        run([(h, k_oth, v_oth, 0, k_oth.shape[0], None) for h in range(group)])

    run([(h, k_own, v_own, 0, diag_start + rows, diag_start) for h in range(group)])


def far_kernel(group, counts, q_ref, acc_in, ml_ref, ka, va, kb, vb, *refs):
    o_ref, s_ref, acc_ref = refs[-3:]
    acc_ref[...] = acc_in[0]

    def put(m_l):
        for h, (_, l) in enumerate(m_l):
            o_t = acc_ref[h] * (1.0 / l)
            o_ref[:, h * HEAD_DIM:(h + 1) * HEAD_DIM] = o_t.T.astype(BF16)

    m_l = [(ml_ref[0, h:h + 1], ml_ref[0, group + h:group + h + 1]) for h in range(group)]

    @pl.when(counts[1] > 0)
    def _():
        n = ka.shape[0]
        put(fold_blocks([(h, k, v, 0, n, None) for k, v in ((ka, va), (kb, vb)) for h in range(group)], q_ref, s_ref, acc_ref, list(m_l)))

    @pl.when(counts[1] == 0)
    def _():
        put(m_l)


def attend_near(counts, q, part, own, other, diag_start, kv_heads, rows):
    width = q.shape[1]
    group = width // HEAD_DIM // kv_heads
    block = own[0].shape[0]
    q_spec = pl.BlockSpec((rows, group * HEAD_DIM), lambda g, c: (part, g))
    kv_spec = pl.BlockSpec((block, HEAD_DIM), lambda g, c: (0, g))
    return pl.pallas_call(
        functools.partial(near_kernel, group, diag_start),
        grid_spec=pltpu.PrefetchScalarGridSpec(
            num_scalar_prefetch=1, grid=(kv_heads,), in_specs=[q_spec] + [kv_spec] * 4,
            out_specs=[pl.BlockSpec((1, group, HEAD_DIM, rows), lambda g, c: (g, 0, 0, 0)), pl.BlockSpec((1, 2 * group, rows), lambda g, c: (g, 0, 0))],
            scratch_shapes=[pltpu.VMEM((2, block, rows), F32)]),
        out_shape=[jax.ShapeDtypeStruct((kv_heads, group, HEAD_DIM, rows), F32), jax.ShapeDtypeStruct((kv_heads, 2 * group, rows), F32)],
        cost_estimate=pl.CostEstimate(flops=4 * rows * width * block, bytes_accessed=8 * rows * width, transcendentals=rows * width // HEAD_DIM * block),
        compiler_params=pltpu.CompilerParams(dimension_semantics=('arbitrary',)),
        name='near',
    )(counts, q, *other, *own)


def attend_far(counts, q, part, near, far0, far1, after, kv_heads, rows):
    width = q.shape[1]
    group = width // HEAD_DIM // kv_heads
    block = far0[0].shape[0]
    q_spec = pl.BlockSpec((rows, group * HEAD_DIM), lambda g, c: (part, g))
    kv_spec = pl.BlockSpec((block, HEAD_DIM), lambda g, c: (0, g))
    return pl.pallas_call(
        functools.partial(far_kernel, group),
        grid_spec=pltpu.PrefetchScalarGridSpec(
            num_scalar_prefetch=1, grid=(kv_heads,),
            in_specs=[q_spec, pl.BlockSpec((1, group, HEAD_DIM, rows), lambda g, c: (g, 0, 0, 0)), pl.BlockSpec((1, 2 * group, rows), lambda g, c: (g, 0, 0))]
            + [kv_spec] * 4 + [pl.BlockSpec(memory_space=pl.ANY)] * len(after),
            out_specs=pl.BlockSpec((rows, group * HEAD_DIM), lambda g, c: (0, g)),
            scratch_shapes=[pltpu.VMEM((2, block, rows), F32), pltpu.VMEM((group, HEAD_DIM, rows), F32)]),
        out_shape=jax.ShapeDtypeStruct((rows, width), BF16),
        cost_estimate=pl.CostEstimate(flops=8 * rows * width * block, bytes_accessed=8 * rows * width, transcendentals=2 * rows * width // HEAD_DIM * block),
        compiler_params=pltpu.CompilerParams(dimension_semantics=('arbitrary',)),
        name='far',
    )(counts, q, *near, *far0, *far1, *after)


def build_kernel(capacity, n_parts, where, slot_ref, gate_ref, *refs):
    parts, (o_ref, pick_ref, scale_ref) = refs[:n_parts], refs[-3:]
    experts, tokens = slot_ref.shape

    @pl.when(pl.program_id(0) == 0)
    def _():
        rank = lax.broadcasted_iota(jnp.int32, (capacity, tokens), 0)
        for e in range(experts):
            hit = slot_ref[e:e + 1, :] == rank
            pick_ref[e * capacity:(e + 1) * capacity, :] = jnp.where(hit, 1.0, 0.0).astype(BF16)
            picked = jnp.sum(jnp.where(hit, gate_ref[e:e + 1, :], 0.0), axis=1, keepdims=True)
            scale_ref[e * capacity:(e + 1) * capacity, :] = jnp.broadcast_to(picked, (capacity, HEAD_DIM))

    for e in range(experts):
        lo, hi, at = e * capacity, (e + 1) * capacity, 0
        total = None
        for part in parts:
            n = part.shape[0]
            term = jnp.dot(pick_ref[lo:hi, at:at + n], part[...], preferred_element_type=F32)
            total = term if total is None else total + term
            at += n
        o_ref[0, 0, e] = (total * scale_ref[lo:hi, 0:1]).astype(BF16)


def build(where, slots, gates, parts, capacity, prior=None, col=512):
    experts, tokens = slots.shape
    d_model = parts[0].shape[1]
    fixed = pl.BlockSpec((experts, tokens), lambda n, w: (0, 0))
    in_specs = [fixed, fixed] + [pl.BlockSpec((p.shape[0], col), lambda n, w: (0, n)) for p in parts]
    args = [slots, gates, *parts]
    aliases = {}
    if prior is not None:
        in_specs.append(pl.BlockSpec(memory_space=pl.ANY))
        args.append(prior)
        aliases = {len(args): 0}
    return pl.pallas_call(
        functools.partial(build_kernel, capacity, len(parts)),
        grid_spec=pltpu.PrefetchScalarGridSpec(
            num_scalar_prefetch=1, grid=(d_model // col,), in_specs=in_specs,
            out_specs=pl.BlockSpec((1, 1, experts, capacity, col), lambda n, w: (0, w[0], 0, 0, n)),
            scratch_shapes=[pltpu.VMEM((experts * capacity, tokens), BF16), pltpu.VMEM((experts * capacity, HEAD_DIM), F32)]),
        out_shape=jax.ShapeDtypeStruct((1, 2, experts, capacity, d_model), BF16),
        input_output_aliases=aliases,
        cost_estimate=pl.CostEstimate(flops=2 * experts * capacity * tokens * d_model, bytes_accessed=2 * d_model * (tokens + experts * capacity), transcendentals=0),
        compiler_params=pltpu.CompilerParams(dimension_semantics=('arbitrary',)),
        name='build',
    )(where, *args)


def slots_of(ids_rows, experts):
    tok_dev = ids_rows.shape[0]
    routed = jnp.any(ids_rows[:, :, None] == jnp.arange(experts)[None, None, :], axis=1)
    earlier = jnp.arange(tok_dev)[None, :] < jnp.arange(tok_dev)[:, None]
    rank = jnp.dot(earlier.astype(BF16), routed.astype(BF16), preferred_element_type=F32)
    return jnp.where(routed, rank, -1.0).astype(jnp.int32).T


def solution(mesh):
    sp_size = mesh.shape['sp']
    ep_size = mesh.shape['ep']
    pairs = [(i, i ^ 1) for i in range(sp_size)]
    across = [(0, 2), (1, 3)]
    ep_same = [(e * sp_size + s, (1 - e) * sp_size + s) for e in range(ep_size) for s in range(sp_size)]
    ep_cross = [(e * sp_size + s, (1 - e) * sp_size + (s ^ 1)) for e in range(ep_size) for s in range(sp_size)]

    def swap(a):
        return lax.ppermute(a, 'sp', pairs)

    def layer(x_blk, w_query, w_key, w_value, w_out, ids_blk, gate_blk):
        x_own = x_blk[0]
        tok_dev, _ = x_own.shape
        half = tok_dev // 2
        chunk = half // 2
        kv_heads = w_key.shape[1] // HEAD_DIM
        experts = gate_blk.shape[2]
        capacity = capacity_of(tok_dev, ids_blk.shape[2], experts)
        ep = lax.axis_index('ep')
        sp = lax.axis_index('sp')

        x_upper = swap(x_own[half:])
        v_own = jnp.dot(x_own, w_value, preferred_element_type=F32).astype(BF16)
        v_a = lax.ppermute(v_own, 'sp', across)
        k_own = jnp.dot(x_own, w_key, preferred_element_type=F32).astype(BF16)
        k_a = lax.ppermute(k_own, 'sp', across)
        k_mate, v_mate = swap(k_own), swap(v_own)
        v_b = swap(v_a)
        k_b = swap(k_a)
        q_low = jnp.dot(x_own[:half], w_query, preferred_element_type=F32).astype(BF16)
        q_upp = jnp.dot(x_upper, w_query, preferred_element_type=F32).astype(BF16)

        far = (sp >= 2).astype(jnp.int32)
        odd = (sp % 2).astype(jnp.int32)
        counts_low = jnp.stack([odd, far])
        counts_upp = jnp.stack([1 - odd, far])

        ids_other = lax.ppermute(ids_blk[0], ('ep', 'sp'), ep_same)
        gates_other = lax.ppermute(gate_blk[0], ('ep', 'sp'), ep_same)
        local = experts // ep_size

        def mine(a):
            return lax.dynamic_slice_in_dim(a, ep * local, local, 0)

        slots_own, gates_own = mine(slots_of(ids_blk[0], experts)), mine(gate_blk[0].T)
        slots_oth, gates_oth = mine(slots_of(ids_other, experts)), mine(gates_other.T)

        near = []
        for c in range(4):
            lower = c < 2
            near.append(attend_near(counts_low if lower else counts_upp, q_low if lower else q_upp, c % 2, (k_own, v_own) if lower else (k_mate, v_mate),
                                    (k_mate, v_mate) if lower else (k_own, v_own), c * chunk, kv_heads, chunk))
        own_rows, other_rows = [], []
        after = [slots_own, gates_own, slots_oth, gates_oth]
        for c in range(4):
            lower = c < 2
            x_c = lax.slice_in_dim(x_own if lower else x_upper, (c % 2) * chunk, (c % 2 + 1) * chunk, axis=0)
            o_c = attend_far(counts_low if lower else counts_upp, q_low if lower else q_upp, c % 2, near[c], (k_a, v_a), (k_b, v_b), after, kv_heads, chunk)
            mixed = jnp.dot(o_c, w_out, preferred_element_type=F32)
            h_c = (x_c.astype(F32) + mixed).astype(BF16)
            after = [h_c]
            own_rows.append(h_c if lower else swap(h_c))
            other_rows.append(lax.ppermute(h_c, ('ep', 'sp'), ep_same if lower else ep_cross))
        hidden = jnp.concatenate(own_rows, axis=0)
        buf = build(ep[None].astype(jnp.int32), slots_own, gates_own, [hidden], capacity)
        buf = build((1 - ep)[None].astype(jnp.int32), slots_oth, gates_oth, other_rows, capacity, prior=buf)
        return hidden[None], buf

    seq_spec = P(('dp', 'ep'), 'sp', None)
    buf_spec = P(('dp', 'sp'), None, 'ep', None, None)
    return jax.shard_map(layer, mesh=mesh, in_specs=(seq_spec, P(), P(), P(), P(), seq_spec, seq_spec), out_specs=(seq_spec, buf_spec), check_vma=False)
```
